128 devices in a mesh: rep: 2 (over core), dp: 64 (over x, y, z).
Axes of the slice: x: 4, y: 4, z: 4, core: 2. Of those that a mesh axis runs over, the one named last changes fastest.
Arguments:
- x: bfloat16 [128, 2048, 1280], P(('rep', 'dp')), parts along dimension 0
- dy: bfloat16 [128, 2048, 1280], P(('rep', 'dp')), parts along dimension 0
- w_gate: bfloat16 [2, 1280, 4480], P(None, 'dp')
- w_up: bfloat16 [2, 1280, 4480], P(None, 'dp')
- w_down: bfloat16 [2, 4480, 1280], P(None, 'dp')
- m_w_gate: float32 [2, 1280, 4480], P(None, 'dp')
- m_w_up: float32 [2, 1280, 4480], P(None, 'dp')
- m_w_down: float32 [2, 4480, 1280], P(None, 'dp')
- v_w_gate: float32 [2, 1280, 4480], P(None, 'dp')
- v_w_up: float32 [2, 1280, 4480], P(None, 'dp')
- v_w_down: float32 [2, 4480, 1280], P(None, 'dp')
Outputs:
- output 1: bfloat16 [4, 1280, 4480], P('rep', 'dp'), parts along dimension 0
- output 2: bfloat16 [4, 1280, 4480], P('rep', 'dp'), parts along dimension 0
- output 3: bfloat16 [4, 4480, 1280], P('rep', 'dp'), parts along dimension 0
- output 4: float32 [4, 1280, 4480], P('rep', 'dp'), parts along dimension 0
- output 5: float32 [4, 1280, 4480], P('rep', 'dp'), parts along dimension 0
- output 6: float32 [4, 4480, 1280], P('rep', 'dp'), parts along dimension 0
- output 7: float32 [4, 1280, 4480], P('rep', 'dp'), parts along dimension 0
- output 8: float32 [4, 1280, 4480], P('rep', 'dp'), parts along dimension 0
- output 9: float32 [4, 4480, 1280], P('rep', 'dp'), parts along dimension 0
There are 2 independent parts. The reference program is written for one: setup_inputs(seed, part) draws one part's arguments, and reference() takes and returns one part's arrays. A program takes and returns all parts, laid end to end along the dimension named above; an argument that names none is the same for every part.
All inputs are finite; a program needn't handle non-finite values.
Results may differ from the reference program's by a relative error of at most 0.0223.
Values are sent between devices in bfloat16 or wider.
A program may use at most 1.5 GiB of HBM per device.

```python
import jax
import jax.numpy as jnp
from jax import lax

SEQUENCES = 64
TOKENS = 2048
D = 1280
FF = 4480
LAYERS = 2
NAMES = ("w_gate", "w_up", "w_down")
SHAPES = {"w_gate": (LAYERS, D, FF), "w_up": (LAYERS, D, FF), "w_down": (LAYERS, FF, D)}


def bump(key, n, height):
    away = (jnp.arange(n, dtype=jnp.int32) - jax.random.randint(key, (), 0, n, jnp.int32)) % n
    return jnp.where(away < n // 8, height, 1.0)


def together(key, own, strength):
    shared = jax.random.normal(key, own.shape[1:], jnp.float32)
    return (own + strength * shared) * lax.rsqrt(1 + strength * strength)


def setup_inputs(seed: int = 0, part: int = 0) -> dict:
    kx, kdy, ka, kb, kz, kf, kh, kl, *keys = jax.random.split(jax.random.key(seed), 8 + 3 * len(NAMES))
    kx, kdy, ka, kb = (jax.random.fold_in(k, part) for k in (kx, kdy, ka, kb))
    kw, km, kv = (keys[i::3] for i in range(3))
    shape = (SEQUENCES, TOKENS, D)
    much_x, much_dy = jax.random.uniform(kz, (2,), jnp.float32, 0.0, 1.0)
    loud = 2.0 ** jax.random.uniform(jax.random.fold_in(kz, 1), (), jnp.float32, -1.0, 2.0)
    layers = 2.0 ** jax.random.uniform(kl, (LAYERS, 1, 1), jnp.float32, -1.0, 1.0)
    x = together(ka, jax.random.normal(kx, shape, jnp.float32), much_x) * bump(kf, D, 4.0)
    dy = together(kb, jax.random.normal(kdy, shape, jnp.float32), much_dy)
    drawn = {"x": x.astype(jnp.bfloat16), "dy": (loud * dy * (SEQUENCES * TOKENS) ** -0.5).astype(jnp.bfloat16)}
    for key, name in zip(kw, NAMES, strict=True):
        w = jax.random.normal(key, SHAPES[name], jnp.float32) * SHAPES[name][1] ** -0.5
        drawn[name] = (w * {"w_gate": 1.0, "w_up": bump(kh, FF, 4.0), "w_down": layers}[name]).astype(jnp.bfloat16)
    for key, name in zip(km, NAMES, strict=True):
        drawn[f"m_{name}"] = 0.1 * jax.random.normal(key, SHAPES[name], jnp.float32)
    for key, name in zip(kv, NAMES, strict=True):
        drawn[f"v_{name}"] = loud * loud * jax.random.uniform(key, SHAPES[name], jnp.float32, 0.05, 0.15)
    return drawn


def matmul(a, w):
    return jnp.dot(a, w, preferred_element_type=jnp.float32).astype(jnp.bfloat16)


def normed(h):
    wide = h.astype(jnp.float32)
    scale = lax.rsqrt(jnp.mean(wide**2, -1, keepdims=True) + 1e-6)
    return (wide * scale).astype(jnp.bfloat16)


def layer(h, w):
    a = normed(h)
    gate = jnp.dot(a, w["w_gate"], preferred_element_type=jnp.float32)
    up = jnp.dot(a, w["w_up"], preferred_element_type=jnp.float32)
    return h + matmul((jax.nn.silu(gate) * up).astype(jnp.bfloat16), w["w_down"])


def adamw(w, m, v, g):
    m = 0.9 * m + 0.1 * g
    v = 0.95 * v + 0.05 * g * g
    step = m * lax.rsqrt(v + 1e-8) + 0.1 * w
    return (w - 0.02 * step).astype(jnp.bfloat16), m, v


def stack(weights, h):
    return lax.scan(lambda h, w: (layer(h, w), None), h, weights)[0]


def reference(x, dy, w_gate, w_up, w_down, m_w_gate, m_w_up, m_w_down, v_w_gate, v_w_up, v_w_down):
    weights = dict(zip(NAMES, (w_gate, w_up, w_down), strict=True))

    def take(so_far, sequence):
        h, by_y = sequence
        _, back = jax.vjp(lambda w: stack(w, h), weights)
        return jax.tree.map(lambda total, term: total + term.astype(jnp.float32), so_far, back(by_y)[0]), None

    none_yet = {name: jnp.zeros(w.shape, jnp.float32) for name, w in weights.items()}
    by_weights, _ = lax.scan(take, none_yet, (x, dy))
    gradients = [by_weights[name].astype(jnp.bfloat16).astype(jnp.float32) for name in NAMES]
    new = [
        adamw(w.astype(jnp.float32), m, v, g)
        for w, m, v, g in zip((w_gate, w_up, w_down), (m_w_gate, m_w_up, m_w_down), (v_w_gate, v_w_up, v_w_down), gradients, strict=True)
    ]
    return tuple(one[which] for which in range(3) for one in new)
```

```python
import jax
import jax.numpy as jnp
from jax import lax
from jax.experimental import pallas as pl
from jax.experimental.pallas import tpu as pltpu
from jax.sharding import PartitionSpec as P


BF, F32 = jnp.bfloat16, jnp.float32
NN, NT = (((1,), (0,)), ((), ())), (((1,), (1,)), ((), ()))
TF = 768
TT = 512
LIMIT = 62 * 1024 * 1024


def dot(a, b, dims=NN):
    return lax.dot_general(a, b, dims, preferred_element_type=F32)


def pieces_of(cols):
    n = cols // 128
    q = [(n + 3 - i) // 4 * 128 for i in range(4)]
    start = [sum(q[:i]) for i in range(4)]
    return [("xy"[i // 2], 1 if i % 2 == 0 else -1, start[i], q[i]) for i in range(4)]


def comm_scratch(rows, cols):
    out = []
    for _, _, _, c in pieces_of(cols):
        out += [pltpu.VMEM((4, rows, c), BF)] * 5 + [pltpu.VMEM((rows, c), BF)] * 4
    return out + [pltpu.SemaphoreType.DMA((4, 6)), pltpu.SemaphoreType.DMA((4, 6)), pltpu.SemaphoreType.DMA((4, 2))]


def comm_events(g_ref, out_ref, scratch):
    _, cols = out_ref.shape
    pieces = pieces_of(cols)
    send, recv, local = scratch[-3:]
    dp = lax.axis_index("dp")
    z = lax.rem(dp, 4)
    pos = {"x": lax.div(dp, 16), "y": lax.rem(lax.div(dp, 4), 4)}

    def near(dim, by):
        at = dict(pos)
        at[dim] = lax.rem(pos[dim] + by + 4, 4)
        return {"dp": at["x"] * 16 + at["y"] * 4 + z}

    def parts(p):
        return scratch[9 * p : 9 * p + 9]

    def part(p, t):
        dim, _, c0, c = pieces[p]
        return g_ref.at[t, :, :, pl.ds(c0, c)] if dim == "x" else g_ref.at[:, t, :, pl.ds(c0, c)]

    def remote(p, k, src, dst, dim, by):
        return pltpu.make_async_remote_copy(
            src_ref=src, dst_ref=dst, send_sem=send.at[p, k], recv_sem=recv.at[p, k], device_id=near(dim, by), device_id_type=pl.DeviceIdType.MESH
        )

    def copies(p):
        dim, s, _, _ = pieces[p]
        other = "y" if dim == "x" else "x"
        i, j = pos[dim], pos[other]
        mod = lambda v: lax.rem(v + 4, 4)
        ra, rs, rr, sm, own, ra2, rs2, rr2, sm2 = parts(p)
        return (
            lambda: remote(p, 0, part(p, mod(i + 2)), ra, dim, s),
            lambda: remote(p, 1, part(p, mod(i - s)), rr, dim, -s),
            lambda: remote(p, 2, sm, rs, dim, s),
            lambda: remote(p, 3, own.at[mod(j + 2)], ra2, other, s),
            lambda: remote(p, 4, own.at[mod(j - s)], rr2, other, -s),
            lambda: remote(p, 5, sm2, rs2, other, s),
            lambda: pltpu.make_async_copy(part(p, mod(i + s)), sm, local.at[p, 0]),
            lambda: pltpu.make_async_copy(part(p, i), own, local.at[p, 1]),
            mod(j + s),
            j,
        )

    def enter():
        barrier = pltpu.get_barrier_semaphore()
        for dim in "xy":
            for by in (1, -1):
                pl.semaphore_signal(barrier, inc=1, device_id=near(dim, by), device_id_type=pl.DeviceIdType.MESH)
        pl.semaphore_wait(barrier, 4)
        for p in range(4):
            c = copies(p)
            c[0]().start()
            c[6]().start()
        for p in range(4):
            c = copies(p)
            c[1]().start()
            c[7]().start()

    def tally(dst, *refs):
        total = refs[0][...].astype(F32)
        for r in refs[1:]:
            total = total + r[...].astype(F32)
        dst[...] = total.astype(BF)

    def over(n, f):
        lax.fori_loop(0, n, lambda k, _: (f(k), 0)[1], 0)

    def first():
        for p in range(4):
            c = copies(p)
            ra, _, _, sm, _, _, _, _, _ = parts(p)
            c[6]().wait()
            c[0]().wait_recv()
            over(4, lambda k: tally(sm.at[k], sm.at[k], ra.at[k]))
            c[2]().start()

    def second():
        for p in range(4):
            c = copies(p)
            _, rs, rr, _, own, _, _, _, _ = parts(p)
            c[7]().wait()
            c[1]().wait_recv()
            c[2]().wait_recv()
            over(4, lambda k: tally(own.at[k], own.at[k], rs.at[k], rr.at[k]))
            c[3]().start()
            c[4]().start()

    def third():
        for p in range(4):
            c = copies(p)
            _, _, _, _, own, ra2, _, _, sm2 = parts(p)
            c[3]().wait_recv()
            tally(sm2, own.at[c[8]], ra2)
            c[5]().start()

    def fourth():
        for p in range(4):
            c = copies(p)
            _, _, c0, w = pieces[p]
            _, _, _, _, own, _, rs2, rr2, _ = parts(p)
            c[4]().wait_recv()
            c[5]().wait_recv()
            tally(out_ref.at[:, pl.ds(c0, w)], own.at[c[9]], rs2, rr2)
            for k in range(6):
                c[k]().wait_send()

    return [enter, first, second, third, fourth]


def run(body, grid, args, in_specs, outs, out_specs, scratch=(), comm=None, at=(), cid=None, flops=0):
    ni, no, ns = len(args), len(outs), len(scratch)
    args, in_specs, outs, out_specs, scratch = list(args), list(in_specs), list(outs), list(out_specs), list(scratch)
    if comm is not None:
        rows, cols = comm.shape[0] // 16, comm.shape[1]
        args.append(comm.reshape(4, 4, rows, cols))
        in_specs.append(pl.BlockSpec(memory_space=pl.ANY))
        outs.append(jax.ShapeDtypeStruct((rows, cols), BF))
        out_specs.append(pl.BlockSpec((rows, cols), lambda *_: (0, 0)))
        scratch += comm_scratch(rows, cols)

    def kernel(*refs):
        ins, rest = refs[:ni], refs[len(args) :]
        os, sc = rest[:no], rest[len(outs) :]
        if comm is not None:
            step = 0
            for d, n in enumerate(grid):
                step = step * n + pl.program_id(d)
            for when, event in zip(at, comm_events(refs[ni], rest[no], sc[ns:])):
                pl.when(step == when)(event)
        if body is not None:
            body(*ins, *os, *sc[:ns])

    params = dict(dimension_semantics=("arbitrary",) * len(grid), vmem_limit_bytes=LIMIT)
    if comm is not None:
        params.update(collective_id=cid, has_side_effects=True)
    return pl.pallas_call(
        kernel,
        grid=grid,
        in_specs=in_specs,
        out_shape=outs,
        out_specs=out_specs,
        scratch_shapes=scratch,
        compiler_params=pltpu.CompilerParams(**params),
        cost_estimate=pl.CostEstimate(flops=flops, bytes_accessed=flops // 500, transcendentals=0),
    )(*args)


def S(shape, dtype=BF):
    return jax.ShapeDtypeStruct(shape, dtype)


def valid(shape, axis, tile, size):
    return lax.broadcasted_iota(jnp.int32, shape, axis) < size - tile * TF


def gate_up_specs(d):
    return [pl.BlockSpec((None, d, TF), lambda j, i, k=k: (k, 0, j)) for k in range(2)]


def joined(w):
    return jnp.concatenate([w[0], w[1]], 1)


def prepared(h):
    t, d = h.shape

    def body(h_ref, a_ref, at_ref):
        wide = h_ref[...].astype(F32)
        scale = lax.rsqrt(jnp.mean(wide * wide, -1, keepdims=True) + 1e-6)
        a = (wide * scale).astype(BF)
        a_ref[...] = a
        at_ref[...] = a.T

    rows = pl.BlockSpec((TT, d), lambda i: (i, 0))
    return run(body, (t // TT,), (h,), [rows], [S((t, d)), S((d, t))], [rows, pl.BlockSpec((d, TT), lambda i: (0, i))], flops=4000 * t)


def act_of(a, wgu):
    (t, d), f = a.shape, wgu.shape[2]
    nf, nt = -(-f // TF), t // TT

    def body(a_ref, g_ref, u_ref, o_ref):
        j = pl.program_id(0)
        gate, up = dot(a_ref[...], g_ref[...]), dot(a_ref[...], u_ref[...])
        act = jax.nn.silu(gate) * up
        o_ref[...] = jnp.where(valid(act.shape, 1, j, f), act, 0.0).astype(BF)

    return run(body, (nf, nt), (a, wgu, wgu), [pl.BlockSpec((TT, d), lambda j, i: (i, 0)), *gate_up_specs(d)], [S((t, nf * TF))], [pl.BlockSpec((TT, TF), lambda j, i: (i, j))], flops=4 * t * d * f)[0]


def down_of(act, wd, h):
    t, d, f = act.shape[0], h.shape[1], wd.shape[1]
    nf, nt = act.shape[1] // TF, t // TT

    def body(a_ref, w_ref, h_ref, o_ref, acc):
        j, i = pl.program_id(0), pl.program_id(1)
        rows = pl.ds(i * TT, TT)

        def add(w):
            got = dot(a_ref[...], w)
            acc[rows, :] = jnp.where(j == 0, got, acc[rows, :] + got)

        @pl.when(j < nf - 1)
        def _():
            add(joined(w_ref))

        @pl.when(j == nf - 1)
        def _():
            add(jnp.where(valid((TF, d), 0, j, f), joined(w_ref), jnp.zeros((), BF)))
            o_ref[...] = (h_ref[...].astype(F32) + acc[rows, :].astype(BF).astype(F32)).astype(BF)

    last = lambda j, i: (jnp.where(j == nf - 1, i, 0), 0)
    return run(
        body, (nf, nt), (act, wd, h),
        [pl.BlockSpec((TT, TF), lambda j, i: (i, j)), pl.BlockSpec((2, TF, d // 2), lambda j, i: (0, j, 0)), pl.BlockSpec((TT, d), last)],
        [S((t, d))], [pl.BlockSpec((TT, d), last)], [pltpu.VMEM((t, d), F32)], flops=2 * t * d * f,
    )[0]


def back_act(a, wgu, dh, wd, **comm):
    (t, d), f = a.shape, wgu.shape[2]
    nf, nt = -(-f // TF), t // TT

    def body(a_ref, g_ref, u_ref, dh_ref, w_ref, at_ref, dg_ref, du_ref):
        j = pl.program_id(0)
        gate, up = dot(a_ref[...], g_ref[...]), dot(a_ref[...], u_ref[...])
        by = dot(dh_ref[...], joined(w_ref), NT).astype(BF).astype(F32)
        s = jax.nn.sigmoid(gate)
        silu = gate * s
        at_ref[...] = (silu * up).astype(BF).T
        ok = valid(by.shape, 1, j, f)
        dg_ref[...] = jnp.where(ok, by * up * (s * (1 + gate * (1 - s))), 0.0).astype(BF)
        du_ref[...] = jnp.where(ok, by * silu, 0.0).astype(BF)

    rows = pl.BlockSpec((TT, d), lambda j, i: (i, 0))
    tile = pl.BlockSpec((TT, TF), lambda j, i: (i, j))
    return run(
        body, (nf, nt), (a, wgu, wgu, dh, wd), [rows, *gate_up_specs(d), rows, pl.BlockSpec((2, TF, d // 2), lambda j, i: (0, j, 0))],
        [S((f, t)), S((t, nf * TF)), S((t, nf * TF))], [pl.BlockSpec((TF, TT), lambda j, i: (j, i)), tile, tile],
        flops=6 * t * d * f, **comm,
    )


def back_in(dg, du, wgu, h, dh, **comm):
    t, (_, d, f) = dg.shape[0], wgu.shape
    nf, nt = dg.shape[1] // TF, t // TT

    def body(dg_ref, du_ref, g_ref, u_ref, h_ref, dh_ref, o_ref, acc):
        j, i = pl.program_id(0), pl.program_id(1)
        rows = pl.ds(i * TT, TT)

        def add(g, u):
            got = dot(dg_ref[...], g, NT) + dot(du_ref[...], u, NT)
            acc[rows, :] = jnp.where(j == 0, got, acc[rows, :] + got)

        @pl.when(j < nf - 1)
        def _():
            add(g_ref[...], u_ref[...])

        @pl.when(j == nf - 1)
        def _():
            ok, zero = valid((d, TF), 1, j, f), jnp.zeros((), BF)
            add(jnp.where(ok, g_ref[...], zero), jnp.where(ok, u_ref[...], zero))
            by = acc[rows, :].astype(BF).astype(F32)
            wide = h_ref[...].astype(F32)
            scale = lax.rsqrt(jnp.mean(wide * wide, -1, keepdims=True) + 1e-6)
            along = jnp.sum(by * wide, -1, keepdims=True)
            own = by * scale - wide * (along * (scale * scale * scale) * (1.0 / d))
            o_ref[...] = (dh_ref[...].astype(F32) + own.astype(BF).astype(F32)).astype(BF)

    last = lambda j, i: (jnp.where(j == nf - 1, i, 0), 0)
    tile, out = pl.BlockSpec((TT, TF), lambda j, i: (i, j)), pl.BlockSpec((TT, d), last)
    return run(body, (nf, nt), (dg, du, wgu, wgu, h, dh), [tile, tile, *gate_up_specs(d), out, out], [S((t, d))], [out], [pltpu.VMEM((t, d), F32)], flops=4 * t * d * f, **comm)


def weights_in(a_t, by, f, **comm):
    d, t = a_t.shape
    nf = by.shape[1] // TF

    def body(a_ref, b_ref, o_ref):
        o_ref[...] = dot(a_ref[...], b_ref[...]).astype(BF)

    return run(body, (nf, 2), (a_t, by), [pl.BlockSpec((d // 2, t), lambda j, i: (i, 0)), pl.BlockSpec((t, TF), lambda j, i: (0, j))], [S((d, f))], [pl.BlockSpec((d // 2, TF), lambda j, i: (i, j))], flops=2 * t * d * f, **comm)


def weights_out(act_t, dh, **comm):
    f, t = act_t.shape
    d, tile = dh.shape[1], 320

    def body(a_ref, b_ref, o_ref):
        o_ref[...] = dot(a_ref[...], b_ref[...]).astype(BF)

    return run(body, (f // tile,), (act_t, dh), [pl.BlockSpec((tile, t), lambda j: (j, 0)), pl.BlockSpec((t, d), lambda j: (0, 0))], [S((f, d))], [pl.BlockSpec((tile, d), lambda j: (j, 0))], flops=2 * t * d * f, **comm)


def only_scatter(g, cid):
    return run(None, (1,), (), [], [], [], comm=g, at=(0,) * 5, cid=cid)[0]


def adamw(w, m, v, g):
    m = 0.9 * m + 0.1 * g
    v = 0.95 * v + 0.05 * g * g
    step = m * lax.rsqrt(v + 1e-8) + 0.1 * w
    return (w - 0.02 * step).astype(BF), m, v


Z_GROUPS = [[4 * k + q for q in range(4)] for k in range(16)]


def solution(mesh):
    def inner(x, dy, *arrays):
        weights, m, v = (arrays[i : i + 3] for i in (0, 3, 6))
        first = lax.axis_index("rep") == 0

        def gate_up(number):
            both = lax.all_gather(jnp.where(first, weights[0][number], weights[1][number]), ("rep", "dp"), axis=0)
            return both.reshape(2, -1, both.shape[-1])

        def down(number):
            w = weights[2][number]
            half = w.shape[1] // 2
            both = lax.all_gather(jnp.where(first, w[:, :half], w[:, half:]), ("rep", "dp"), axis=0)
            return both.reshape(2, -1, half)

        wgu0 = gate_up(0)
        wd0 = down(0)
        wgu1 = gate_up(1)
        wd1 = down(1)
        f = wgu0.shape[2]
        h0, dh2 = x[0], dy[0]
        a0, a0_t = prepared(h0)
        h1 = down_of(act_of(a0, wgu0), wd0, h0)
        a1, a1_t = prepared(h1)
        at1, dg1, du1 = back_act(a1, wgu1, dh2, wd1)
        down1 = weights_out(at1, dh2)[0]
        gate1 = weights_in(a1_t, dg1, f)[0]
        up1, s_down1 = weights_in(a1_t, du1, f, comm=down1, at=(0, 3, 9, 10, 11), cid=1)
        dh1, s_gate1 = back_in(dg1, du1, wgu1, h1, dh2, comm=gate1, at=(0, 6, 18, 21, 23), cid=2)
        at0, dg0, du0, s_up1 = back_act(a0, wgu0, dh1, wd0, comm=up1, at=(0, 6, 17, 20, 23), cid=3)
        gate0 = weights_in(a0_t, dg0, f)[0]
        up0, s_gate0 = weights_in(a0_t, du0, f, comm=gate0, at=(0, 3, 9, 10, 11), cid=4)
        down0, s_up0 = weights_out(at0, dh1, comm=up0, at=(0, 3, 11, 12, 13), cid=5)
        s_down0 = only_scatter(down0, 6)
        found = [(s_gate0, s_up0, s_down0), (s_gate1, s_up1, s_down1)]
        gradients = []
        for i in range(3):
            by_layer = []
            for of in found:
                terms = of[i].reshape(4, -1, of[i].shape[1])
                terms = lax.all_to_all(terms, "dp", 0, 0, axis_index_groups=Z_GROUPS)
                t = [terms[k].astype(F32) for k in range(4)]
                by_layer.append(((t[0] + t[1]) + (t[2] + t[3])).astype(BF).astype(F32))
            gradients.append(jnp.stack(by_layer))
        new = [adamw(w.astype(F32), m, v, g) for w, m, v, g in zip(weights, m, v, gradients, strict=True)]
        return tuple(one[which] for which in range(3) for one in new)

    states, cut = P(("rep", "dp"), None, None), P(None, "dp", None)
    return jax.shard_map(
        inner,
        mesh=mesh,
        in_specs=(states, states) + (cut,) * 9,
        out_specs=(P("rep", "dp", None),) * 9,
        check_vma=False,
    )
```

```python
import jax
import jax.numpy as jnp
from jax import lax
from jax.experimental import pallas as pl
from jax.experimental.pallas import tpu as pltpu
from jax.sharding import PartitionSpec as P

BF, F32 = jnp.bfloat16, jnp.float32
NN, NT = (((1,), (0,)), ((), ())), (((1,), (1,)), ((), ()))
TF = 768
TT = 512
LIMIT = 62 * 1024 * 1024


def dot(a, b, dims=NN):
    return lax.dot_general(a, b, dims, preferred_element_type=F32)


MESH = pl.DeviceIdType.MESH


def mod(v):
    return lax.rem(v + 4, 4)


def place():
    dp = lax.axis_index("dp")
    return {"x": lax.div(dp, 16), "y": lax.rem(lax.div(dp, 4), 4), "z": lax.rem(dp, 4)}


def near(dim, by):
    at = place()
    at[dim] = mod(at[dim] + by)
    return {"dp": at["x"] * 16 + at["y"] * 4 + at["z"]}


def peer():
    return {"rep": 1 - lax.axis_index("rep")}


def greet():
    barrier = pltpu.get_barrier_semaphore()
    for where in [near(d, by) for d in "xy" for by in (1, -1)] + [near("z", by) for by in (1, 2, 3)] + [peer()]:
        pl.semaphore_signal(barrier, inc=1, device_id=where, device_id_type=MESH)
    pl.semaphore_wait(barrier, 8)


def remote(sems, k, src, dst, where):
    send, recv = sems
    return pltpu.make_async_remote_copy(src_ref=src, dst_ref=dst, send_sem=send.at[k], recv_sem=recv.at[k], device_id=where, device_id_type=MESH)


def pieces_of(cols):
    n = cols // 128
    q = [(n + 3 - i) // 4 * 128 for i in (0, 2, 1, 3)]
    return [("xy"[i // 2], "yx"[i // 2], 1 if i % 2 == 0 else -1, sum(q[:i]), q[i]) for i in range(4)]


class Scatter:
    def __init__(self, g, at):
        rows, cols = g.shape[0] // 16, g.shape[1]
        self.at, self.pieces = at, pieces_of(cols)
        self.args, self.specs = [g.reshape(4, 4, rows, cols)], [pl.BlockSpec(memory_space=pl.ANY)]
        own = (rows // 4, cols)
        self.outs, self.out_specs = [jax.ShapeDtypeStruct(own, BF)], [pl.BlockSpec(own, lambda *_: (0, 0))]
        self.scratch = []
        for *_, c in self.pieces:
            self.scratch += [pltpu.VMEM((4, rows, c), BF)] * 5 + [pltpu.VMEM((2, rows, c), F32)] + [pltpu.VMEM((rows, c), BF)] * 4
        self.scratch += [pltpu.VMEM((rows, cols), F32), pltpu.VMEM((4, *own), BF), pltpu.VMEM((4, *own), BF), pltpu.VMEM(own, F32)]
        self.scratch += [pltpu.SemaphoreType.DMA((27,)), pltpu.SemaphoreType.DMA((27,)), pltpu.SemaphoreType.DMA((8,))]

    def events(self, ins, outs, scratch):
        (g_ref,), (out_ref,) = ins, outs
        total, z_send, z_recv, z_own, send, recv, local = scratch[40:]
        sems, pos, r = (send, recv), place(), out_ref.shape[0]

        def part(p, t):
            dim, _, _, c0, c = self.pieces[p]
            return g_ref.at[t, :, :, pl.ds(c0, c)] if dim == "x" else g_ref.at[:, t, :, pl.ds(c0, c)]

        def copy(p, k):
            a, b, s, _, _ = self.pieces[p]
            i, j = pos[a], pos[b]
            ra, rs, rr, sm, own, _, ra2, rs2, rr2, sm2 = scratch[10 * p : 10 * p + 10]
            n = 6 * p + k
            if k == 0:
                return remote(sems, n, part(p, mod(i + 2)), ra, near(a, s))
            if k == 1:
                return remote(sems, n, part(p, mod(i - s)), rr, near(a, -s))
            if k == 2:
                return remote(sems, n, sm, rs, near(a, s))
            if k == 3:
                return remote(sems, n, own.at[mod(j + 2)], ra2, near(b, s))
            if k == 4:
                return remote(sems, n, own.at[mod(j - s)], rr2, near(b, -s))
            if k == 5:
                return remote(sems, n, sm2, rs2, near(b, s))
            if k == 6:
                return pltpu.make_async_copy(part(p, mod(i + s)), sm, local.at[2 * p])
            return pltpu.make_async_copy(part(p, i), own, local.at[2 * p + 1])

        def along_z(k):
            return remote(sems, 23 + k, z_send.at[mod(pos["z"] + k)], z_recv.at[k], near("z", k))

        def wide(ref):
            return ref[...].astype(F32)

        def zero():
            for p in range(4):
                copy(p, 0).start()
                copy(p, 6).start()
            for p in range(4):
                copy(p, 1).start()
                copy(p, 7).start()

        def first():
            for p in range(4):
                ra, _, _, sm = scratch[10 * p : 10 * p + 4]
                copy(p, 6).wait()
                copy(p, 0).wait_recv()

                def add(k, _, sm=sm, ra=ra):
                    sm[k] = (wide(sm.at[k]) + wide(ra.at[k])).astype(BF)
                    return 0

                lax.fori_loop(0, 4, add, 0)
                copy(p, 2).start()

        def second():
            for p in range(4):
                _, b, s, _, _ = self.pieces[p]
                _, rs, rr, _, own, kept = scratch[10 * p : 10 * p + 6]
                copy(p, 7).wait()
                copy(p, 1).wait_recv()
                copy(p, 2).wait_recv()
                for k in (2, 3, 0, 1):
                    t = mod(pos[b] + (k * s) % 4)
                    found = wide(own.at[t]) + wide(rs.at[t]) + wide(rr.at[t])
                    if k < 2:
                        kept[k] = found
                    else:
                        own[t] = found.astype(BF)
                copy(p, 3).start()
                copy(p, 4).start()

        def third():
            for p in range(4):
                kept, ra2, _, _, sm2 = scratch[10 * p + 5 : 10 * p + 10]
                copy(p, 3).wait_recv()
                sm2[...] = (kept[1] + wide(ra2)).astype(BF)
                copy(p, 5).start()

        def fourth():
            for p in range(4):
                _, _, _, c0, c = self.pieces[p]
                kept, _, rs2, rr2, _ = scratch[10 * p + 5 : 10 * p + 10]
                copy(p, 4).wait_recv()
                copy(p, 5).wait_recv()
                total[:, pl.ds(c0, c)] = kept[0] + wide(rs2) + wide(rr2)
            for q in range(4):
                found = total[pl.ds(r * q, r), :]
                z_send[q] = found.astype(BF)

                @pl.when(pos["z"] == q)
                def _(found=found):
                    z_own[...] = found

            for k in (1, 2, 3):
                along_z(k).start()

        def fifth():
            for k in (1, 2, 3):
                along_z(k).wait_recv()
            out_ref[...] = (z_own[...] + wide(z_recv.at[1]) + (wide(z_recv.at[2]) + wide(z_recv.at[3]))).astype(BF)
            for k in (1, 2, 3):
                along_z(k).wait_send()
            for p in range(4):
                for k in range(6):
                    copy(p, k).wait_send()

        return [zero, first, second, third, fourth, fifth]


class Fetch:
    def __init__(self, mine, at):
        r, cols = mine.shape
        self.at, self.pieces = at, pieces_of(cols)
        self.args, self.specs = [mine], [pl.BlockSpec((r, cols), lambda *_: (0, 0))]
        self.outs, self.out_specs = [jax.ShapeDtypeStruct((2, 4, 4, 4 * r, cols), BF)], [pl.BlockSpec(memory_space=pl.ANY)]
        self.scratch = [pltpu.VMEM((4, r, cols), BF), pltpu.VMEM((4 * r, cols), F32), pltpu.VMEM((4 * r, cols), BF)]
        self.scratch += [pltpu.SemaphoreType.DMA((43,)), pltpu.SemaphoreType.DMA((43,)), pltpu.SemaphoreType.DMA((1,))]

    def events(self, ins, outs, scratch):
        (mine,), (w,) = ins, outs
        four, wide, block, send, recv, local = scratch
        sems, pos, r = (send, recv), place(), mine.shape[0]
        which = lax.axis_index("rep")

        def one(p, t):
            a, _, _, c0, c = self.pieces[p]
            return w.at[which, t, pos["y"], :, pl.ds(c0, c)] if a == "x" else w.at[which, pos["x"], t, :, pl.ds(c0, c)]

        def row(p, t):
            a, _, _, c0, c = self.pieces[p]
            return w.at[which, :, t, :, pl.ds(c0, c)] if a == "x" else w.at[which, t, :, :, pl.ds(c0, c)]

        def copy(p, k):
            a, b, s, _, _ = self.pieces[p]
            if k < 3:
                ref, where = one(p, mod(pos[a] + (0, 0, -s)[k])), near(a, (1, -1, s)[k])
            elif k < 6:
                ref, where = row(p, mod(pos[b] + (0, 0, -s)[k - 3])), near(b, (1, -1, s)[k - 3])
            else:
                ref, where = row(p, mod(pos[b] + (0, 1, -1, 2)[k - 6])), peer()
            return remote(sems, 10 * p + k, ref, ref, where)

        def along_z(k):
            return remote(sems, 39 + k, mine, four.at[pos["z"]], near("z", k))

        def zero():
            for k in (1, 2, 3):
                along_z(k).start()
            four[pos["z"]] = mine[...]

        def first():
            for k in (1, 2, 3):
                along_z(k).wait_recv()
            for q in range(4):
                wide[pl.ds(r * q, r), :] = four[q].astype(F32)
            block[...] = wide[...].astype(BF)
            own = pltpu.make_async_copy(block, w.at[which, pos["x"], pos["y"]], local.at[0])
            own.start()
            own.wait()
            for p in range(4):
                copy(p, 0).start()
                copy(p, 1).start()

        def second():
            for p in range(4):
                copy(p, 0 if self.pieces[p][2] > 0 else 1).wait_recv()
                copy(p, 2).start()

        def third():
            for p in range(4):
                copy(p, 1 if self.pieces[p][2] > 0 else 0).wait_recv()
                copy(p, 2).wait_recv()
                for k in (3, 4, 6):
                    copy(p, k).start()

        def fourth():
            for p in range(4):
                up = self.pieces[p][2] > 0
                copy(p, 3 if up else 4).wait_recv()
                copy(p, 5).start()
                copy(p, 8 if up else 7).start()

        def fifth():
            for p in range(4):
                up = self.pieces[p][2] > 0
                copy(p, 4 if up else 3).wait_recv()
                copy(p, 7 if up else 8).start()
            for p in range(4):
                copy(p, 5).wait_recv()
                copy(p, 9).start()

        def sixth():
            for k in (1, 2, 3):
                along_z(k).wait_send()
            for p in range(4):
                for k in range(6, 10):
                    copy(p, k).wait_recv()
                for k in range(10):
                    copy(p, k).wait_send()

        return [zero, first, second, third, fourth, fifth, sixth]


def run(body, grid, args, in_specs, outs, out_specs, scratch=(), comms=(), cid=None, flops=0, name=None):
    ni, no, ns = len(args), len(outs), len(scratch)
    args, in_specs, outs, out_specs, scratch = list(args), list(in_specs), list(outs), list(out_specs), list(scratch)
    spans = []
    for one in comms:
        lengths = [len(v) for v in (args, outs, scratch)]
        args += one.args
        in_specs += one.specs
        outs += one.outs
        out_specs += one.out_specs
        scratch += one.scratch
        spans.append([slice(lo, len(v)) for lo, v in zip(lengths, (args, outs, scratch))])

    def kernel(*refs):
        ins, os, sc = refs[: len(args)], refs[len(args) : len(args) + len(outs)], refs[len(args) + len(outs) :]
        step = 0
        for d, n in enumerate(grid):
            step = step * n + pl.program_id(d)
        todo = []
        for one, (i, o, c) in zip(comms, spans):
            todo.append(list(zip(one.at, one.events(ins[i], os[o], sc[c]), strict=True)))
        if comms:
            pl.when(step == 0)(greet)
        for n in range(max([len(t) for t in todo], default=0)):
            for t in todo:
                if n < len(t):
                    pl.when(step == t[n][0])(t[n][1])
        if body is not None:
            body(*ins[:ni], *os[:no], *sc[:ns])

    params = dict(dimension_semantics=("arbitrary",) * len(grid), vmem_limit_bytes=LIMIT)
    if comms:
        params.update(collective_id=cid, has_side_effects=True)
    return pl.pallas_call(
        kernel,
        grid=grid,
        in_specs=in_specs,
        out_shape=outs,
        out_specs=out_specs,
        scratch_shapes=scratch,
        compiler_params=pltpu.CompilerParams(**params),
        cost_estimate=pl.CostEstimate(flops=flops, bytes_accessed=flops // 500, transcendentals=0),
        name=name,
    )(*args)


def S(shape, dtype=BF):
    return jax.ShapeDtypeStruct(shape, dtype)


def valid(shape, axis, tile, size):
    return lax.broadcasted_iota(jnp.int32, shape, axis) < size - tile * TF


def gate_up_specs(d):
    return [pl.BlockSpec((None, d, TF), lambda j, i, k=k: (k, 0, j)) for k in range(2)]


def prepared(h):
    t, d = h.shape

    def body(h_ref, a_ref, at_ref):
        wide = h_ref[...].astype(F32)
        scale = lax.rsqrt(jnp.mean(wide * wide, -1, keepdims=True) + 1e-6)
        a = (wide * scale).astype(BF)
        a_ref[...] = a
        at_ref[...] = a.T

    rows = pl.BlockSpec((TT, d), lambda i: (i, 0))
    return run(body, (t // TT,), (h,), [rows], [S((t, d)), S((d, t))], [rows, pl.BlockSpec((d, TT), lambda i: (0, i))], flops=4000 * t, name="prepared")


def act_of(a, wgu, **comm):
    (t, d), f = a.shape, wgu.shape[2]
    nf, tile = -(-f // TF), 2 * TT

    def body(a_ref, g_ref, u_ref, o_ref):
        j = pl.program_id(0)
        for k in range(2):
            rows = pl.ds(k * TT, TT)
            gate, up = dot(a_ref[rows, :], g_ref[...]), dot(a_ref[rows, :], u_ref[...])
            act = jax.nn.silu(gate) * up
            o_ref[rows, :] = jnp.where(valid(act.shape, 1, j, f), act, 0.0).astype(BF)

    return run(body, (nf, t // tile), (a, wgu, wgu), [pl.BlockSpec((tile, d), lambda j, i: (i, 0)), *gate_up_specs(d)], [S((t, nf * TF))], [pl.BlockSpec((tile, TF), lambda j, i: (i, j))], flops=4 * t * d * f, name="act", **comm)


def down_of(act, wd, number, h, **comm):
    t, d, f = act.shape[0], h.shape[1], wd.shape[1]
    nf, nt = act.shape[1] // TF, t // TT

    def body(a_ref, w_ref, h_ref, o_ref, acc):
        j, i = pl.program_id(0), pl.program_id(1)
        rows = pl.ds(i * TT, TT)

        def add(w):
            got = dot(a_ref[...], w)
            acc[rows, :] = jnp.where(j == 0, got, acc[rows, :] + got)

        @pl.when(j < nf - 1)
        def _():
            add(w_ref[...])

        @pl.when(j == nf - 1)
        def _():
            add(jnp.where(valid((TF, d), 0, j, f), w_ref[...], jnp.zeros((), BF)))
            o_ref[...] = (h_ref[...].astype(F32) + acc[rows, :].astype(BF).astype(F32)).astype(BF)

    last = lambda j, i: (jnp.where(j == nf - 1, i, 0), 0)
    return run(
        body, (nf, nt), (act, wd, h),
        [pl.BlockSpec((TT, TF), lambda j, i: (i, j)), pl.BlockSpec((None, TF, d), lambda j, i: (number, j, 0)), pl.BlockSpec((TT, d), last)],
        [S((t, d))], [pl.BlockSpec((TT, d), last)], [pltpu.VMEM((t, d), F32)], flops=2 * t * d * f, name="down", **comm,
    )


def back_act(a, wgu, dh, wd, number, tile=TT, **comm):
    (t, d), f = a.shape, wgu.shape[2]
    nf = -(-f // TF)

    def body(a_ref, g_ref, u_ref, dh_ref, w_ref, at_ref, dg_ref, du_ref):
        j = pl.program_id(0)
        for k in range(tile // TT):
            rows = pl.ds(k * TT, TT)
            gate, up = dot(a_ref[rows, :], g_ref[...]), dot(a_ref[rows, :], u_ref[...])
            by = dot(dh_ref[rows, :], w_ref[...], NT).astype(BF).astype(F32)
            s = jax.nn.sigmoid(gate)
            silu = gate * s
            at_ref[:, rows] = (silu * up).astype(BF).T
            ok = valid(by.shape, 1, j, f)
            dg_ref[rows, :] = jnp.where(ok, by * up * (s * (1 + gate * (1 - s))), 0.0).astype(BF)
            du_ref[rows, :] = jnp.where(ok, by * silu, 0.0).astype(BF)

    rows = pl.BlockSpec((tile, d), lambda j, i: (i, 0))
    out = pl.BlockSpec((tile, TF), lambda j, i: (i, j))
    return run(
        body, (nf, t // tile), (a, wgu, wgu, dh, wd), [rows, *gate_up_specs(d), rows, pl.BlockSpec((None, TF, d), lambda j, i: (number, j, 0))],
        [S((f, t)), S((t, nf * TF)), S((t, nf * TF))], [pl.BlockSpec((TF, tile), lambda j, i: (j, i)), out, out],
        flops=6 * t * d * f, name="back_act", **comm,
    )


def back_in(dg, du, wgu, h, dh, **comm):
    t, (_, d, f) = dg.shape[0], wgu.shape
    nf, nt = dg.shape[1] // TF, t // TT

    def body(dg_ref, du_ref, g_ref, u_ref, h_ref, dh_ref, o_ref, acc):
        j, i = pl.program_id(0), pl.program_id(1)
        rows = pl.ds(i * TT, TT)

        def add(g, u):
            got = dot(dg_ref[...], g, NT) + dot(du_ref[...], u, NT)
            acc[rows, :] = jnp.where(j == 0, got, acc[rows, :] + got)

        @pl.when(j < nf - 1)
        def _():
            add(g_ref[...], u_ref[...])

        @pl.when(j == nf - 1)
        def _():
            ok, zero = valid((d, TF), 1, j, f), jnp.zeros((), BF)
            add(jnp.where(ok, g_ref[...], zero), jnp.where(ok, u_ref[...], zero))
            by = acc[rows, :].astype(BF).astype(F32)
            wide = h_ref[...].astype(F32)
            scale = lax.rsqrt(jnp.mean(wide * wide, -1, keepdims=True) + 1e-6)
            along = jnp.sum(by * wide, -1, keepdims=True)
            own = by * scale - wide * (along * (scale * scale * scale) * (1.0 / d))
            o_ref[...] = (dh_ref[...].astype(F32) + own.astype(BF).astype(F32)).astype(BF)

    last = lambda j, i: (jnp.where(j == nf - 1, i, 0), 0)
    tile, out = pl.BlockSpec((TT, TF), lambda j, i: (i, j)), pl.BlockSpec((TT, d), last)
    return run(body, (nf, nt), (dg, du, wgu, wgu, h, dh), [tile, tile, *gate_up_specs(d), out, out], [S((t, d))], [out], [pltpu.VMEM((t, d), F32)], flops=4 * t * d * f, name="back_in", **comm)


def weights_in(a_t, dg, du, f, **comm):
    d, t = a_t.shape
    nf, half = dg.shape[1] // TF, d // 2

    def body(a_ref, g_ref, u_ref, og_ref, ou_ref):
        @pl.when(pl.program_id(0) < nf)
        def _():
            og_ref[...] = dot(a_ref[...], g_ref[...]).astype(BF)

        @pl.when(pl.program_id(0) >= nf)
        def _():
            ou_ref[...] = dot(a_ref[...], u_ref[...]).astype(BF)

    gate = lambda j: jnp.minimum(j, nf - 1)
    up = lambda j: jnp.maximum(j - nf, 0)
    return run(
        body, (2 * nf, 2), (a_t, dg, du),
        [pl.BlockSpec((half, t), lambda j, i: (i, 0)), pl.BlockSpec((t, TF), lambda j, i: (0, gate(j))), pl.BlockSpec((t, TF), lambda j, i: (0, up(j)))],
        [S((d, f)), S((d, f))],
        [pl.BlockSpec((half, TF), lambda j, i: (jnp.where(j < nf, i, 1), gate(j))), pl.BlockSpec((half, TF), lambda j, i: (jnp.where(j < nf, 0, i), up(j)))],
        flops=4 * t * d * f, name="weights_in", **comm,
    )


def weights_out(act_t, dh, **comm):
    f, t = act_t.shape
    d, tile = dh.shape[1], 320

    def body(a_ref, b_ref, o_ref):
        o_ref[...] = dot(a_ref[...], b_ref[...]).astype(BF)

    return run(body, (f // tile,), (act_t, dh), [pl.BlockSpec((tile, t), lambda j: (j, 0)), pl.BlockSpec((t, d), lambda j: (0, 0))], [S((f, d))], [pl.BlockSpec((tile, d), lambda j: (j, 0))], flops=2 * t * d * f, name="weights_out", **comm)


NAMES = ("w_gate", "w_up", "w_down")


def normed(h):
    wide = h.astype(F32)
    scale = lax.rsqrt(jnp.mean(wide**2, -1, keepdims=True) + 1e-6)
    return (wide * scale).astype(BF)


def adamw(w, m, v, g):
    m = 0.9 * m + 0.1 * g
    v = 0.95 * v + 0.05 * g * g
    step = m * lax.rsqrt(v + 1e-8) + 0.1 * w
    return (w - 0.02 * step).astype(BF), m, v


def solution(mesh):
    def step(x, dy, *arrays):
        weights, m, v = (arrays[i : i + 3] for i in (0, 3, 6))
        first = lax.axis_index("rep") == 0
        f = weights[0].shape[2]

        def gate_up(number, at):
            return Fetch(jnp.where(first, weights[0][number], weights[1][number]), at)

        def whole(w):
            return w.reshape(2, -1, w.shape[-1])

        downs = Fetch(jnp.where(first, weights[2][0], weights[2][1]), (0, 2, 4, 5, 10, 11, 11))
        h0, dh2 = x[0], dy[0]
        (wgu0,) = run(None, (1,), (), [], [], [], comms=[gate_up(0, (0,) * 7)], cid=1, name="fetch")
        wgu0 = whole(wgu0)
        a0, a0_t = prepared(h0)
        act0, wd = act_of(a0, wgu0, comms=[downs], cid=2)
        wd = whole(wd)
        h1, wgu1 = down_of(act0, wd, 0, h0, comms=[gate_up(1, (0, 5, 10, 14, 23, 23, 23))], cid=3)
        wgu1 = whole(wgu1)
        a1, a1_t = prepared(h1)
        at1, dg1, du1 = back_act(a1, wgu1, dh2, wd, 1, 2 * TT)
        down1 = weights_out(at1, dh2)[0]
        gate1, up1, g_down1 = weights_in(a1_t, dg1, du1, f, comms=[Scatter(down1, (0, 6, 17, 20, 22, 23))], cid=4)
        dh1, g_gate1 = back_in(dg1, du1, wgu1, h1, dh2, comms=[Scatter(gate1, (0, 6, 17, 20, 22, 23))], cid=5)
        at0, dg0, du0, g_up1 = back_act(a0, wgu0, dh1, wd, 0, comms=[Scatter(up1, (0, 5, 14, 18, 20, 22))], cid=6)
        down0 = weights_out(at0, dh1)[0]
        gate0, up0, g_down0 = weights_in(a0_t, dg0, du0, f, comms=[Scatter(down0, (0, 6, 17, 20, 22, 23))], cid=7)
        g_gate0, g_up0 = run(None, (1,), (), [], [], [], comms=[Scatter(gate0, (0,) * 6), Scatter(up0, (0,) * 6)], cid=8, name="scatter")
        gradients = [jnp.stack(pair).astype(F32) for pair in ((g_gate0, g_gate1), (g_up0, g_up1), (g_down0, g_down1))]
        new = [adamw(w.astype(F32), m, v, g) for w, m, v, g in zip(weights, m, v, gradients, strict=True)]
        return tuple(one[which] for which in range(3) for one in new)

    states, cut = P(("rep", "dp"), None, None), P(None, "dp", None)
    return jax.shard_map(
        step,
        mesh=mesh,
        in_specs=(states, states) + (cut,) * 9,
        out_specs=(P("rep", "dp", None),) * 9,
        check_vma=False,
    )
```

```python
import jax
import jax.numpy as jnp
from jax import lax
from jax.experimental import pallas as pl
from jax.experimental.pallas import tpu as pltpu
from jax.sharding import PartitionSpec as P

BF, F32 = jnp.bfloat16, jnp.float32
NN, NT = (((1,), (0,)), ((), ())), (((1,), (1,)), ((), ()))
TF = 768
TT = 512
LIMIT = 62 * 1024 * 1024


def dot(a, b, dims=NN):
    return lax.dot_general(a, b, dims, preferred_element_type=F32)


MESH = pl.DeviceIdType.MESH


def mod(v):
    return lax.rem(v + 4, 4)


def place():
    dp = lax.axis_index("dp")
    return {"x": lax.div(dp, 16), "y": lax.rem(lax.div(dp, 4), 4), "z": lax.rem(dp, 4)}


def near(dim, by):
    at = place()
    at[dim] = mod(at[dim] + by)
    return {"dp": at["x"] * 16 + at["y"] * 4 + at["z"]}


def peer():
    return {"rep": 1 - lax.axis_index("rep")}


def greet():
    barrier = pltpu.get_barrier_semaphore()
    for where in [near(d, by) for d in "xy" for by in (1, -1)] + [near("z", by) for by in (1, 2, 3)] + [peer()]:
        pl.semaphore_signal(barrier, inc=1, device_id=where, device_id_type=MESH)
    pl.semaphore_wait(barrier, 8)


def remote(sems, k, src, dst, where):
    send, recv = sems
    return pltpu.make_async_remote_copy(src_ref=src, dst_ref=dst, send_sem=send.at[k], recv_sem=recv.at[k], device_id=where, device_id_type=MESH)


def pieces_of(cols):
    n = cols // 128
    q = [(n + 3 - i) // 4 * 128 for i in (0, 2, 1, 3)]
    return [("xy"[i // 2], "yx"[i // 2], 1 if i % 2 == 0 else -1, sum(q[:i]), q[i]) for i in range(4)]


class Scatter:
    def __init__(self, g, at):
        rows, cols = g.shape[0] // 16, g.shape[1]
        self.at, self.pieces = at, pieces_of(cols)
        self.args, self.specs = [g.reshape(4, 4, rows, cols)], [pl.BlockSpec(memory_space=pl.ANY)]
        own = (rows // 4, cols)
        self.outs, self.out_specs = [jax.ShapeDtypeStruct(own, BF)], [pl.BlockSpec(own, lambda *_: (0, 0))]
        self.scratch = []
        for *_, c in self.pieces:
            self.scratch += [pltpu.VMEM((4, rows, c), BF)] * 5 + [pltpu.VMEM((2, rows, c), F32)] + [pltpu.VMEM((rows, c), BF)] * 4
        self.scratch += [pltpu.VMEM((rows, cols), F32), pltpu.VMEM((4, *own), BF), pltpu.VMEM((4, *own), BF), pltpu.VMEM(own, F32)]
        self.scratch += [pltpu.SemaphoreType.DMA((27,)), pltpu.SemaphoreType.DMA((27,)), pltpu.SemaphoreType.DMA((8,))]

    def events(self, ins, outs, scratch):
        (g_ref,), (out_ref,) = ins, outs
        total, z_send, z_recv, z_own, send, recv, local = scratch[40:]
        sems, pos, r = (send, recv), place(), out_ref.shape[0]

        def part(p, t):
            dim, _, _, c0, c = self.pieces[p]
            return g_ref.at[t, :, :, pl.ds(c0, c)] if dim == "x" else g_ref.at[:, t, :, pl.ds(c0, c)]

        def copy(p, k):
            a, b, s, _, _ = self.pieces[p]
            i, j = pos[a], pos[b]
            ra, rs, rr, sm, own, _, ra2, rs2, rr2, sm2 = scratch[10 * p : 10 * p + 10]
            n = 6 * p + k
            if k == 0:
                return remote(sems, n, part(p, mod(i + 2)), ra, near(a, s))
            if k == 1:
                return remote(sems, n, part(p, mod(i - s)), rr, near(a, -s))
            if k == 2:
                return remote(sems, n, sm, rs, near(a, s))
            if k == 3:
                return remote(sems, n, own.at[mod(j + 2)], ra2, near(b, s))
            if k == 4:
                return remote(sems, n, own.at[mod(j - s)], rr2, near(b, -s))
            if k == 5:
                return remote(sems, n, sm2, rs2, near(b, s))
            if k == 6:
                return pltpu.make_async_copy(part(p, mod(i + s)), sm, local.at[2 * p])
            return pltpu.make_async_copy(part(p, i), own, local.at[2 * p + 1])

        def along_z(k):
            return remote(sems, 23 + k, z_send.at[mod(pos["z"] + k)], z_recv.at[k], near("z", k))

        def wide(ref):
            return ref[...].astype(F32)

        def zero():
            for p in range(4):
                copy(p, 0).start()
                copy(p, 6).start()
            for p in range(4):
                copy(p, 1).start()
                copy(p, 7).start()

        def first():
            for p in range(4):
                ra, _, _, sm = scratch[10 * p : 10 * p + 4]
                copy(p, 6).wait()
                copy(p, 0).wait_recv()

                def add(k, _, sm=sm, ra=ra):
                    sm[k] = (wide(sm.at[k]) + wide(ra.at[k])).astype(BF)
                    return 0

                lax.fori_loop(0, 4, add, 0)
                copy(p, 2).start()

        def second():
            for p in range(4):
                _, b, s, _, _ = self.pieces[p]
                _, rs, rr, _, own, kept = scratch[10 * p : 10 * p + 6]
                copy(p, 7).wait()
                copy(p, 1).wait_recv()
                copy(p, 2).wait_recv()
                for k in (2, 3, 0, 1):
                    t = mod(pos[b] + (k * s) % 4)
                    found = wide(own.at[t]) + wide(rs.at[t]) + wide(rr.at[t])
                    if k < 2:
                        kept[k] = found
                    else:
                        own[t] = found.astype(BF)
                copy(p, 3).start()
                copy(p, 4).start()

        def third():
            for p in range(4):
                kept, ra2, _, _, sm2 = scratch[10 * p + 5 : 10 * p + 10]
                copy(p, 3).wait_recv()
                sm2[...] = (kept[1] + wide(ra2)).astype(BF)
                copy(p, 5).start()

        def fourth():
            for p in range(4):
                _, _, _, c0, c = self.pieces[p]
                kept, _, rs2, rr2, _ = scratch[10 * p + 5 : 10 * p + 10]
                copy(p, 4).wait_recv()
                copy(p, 5).wait_recv()
                total[:, pl.ds(c0, c)] = kept[0] + wide(rs2) + wide(rr2)
            for q in range(4):
                found = total[pl.ds(r * q, r), :]
                z_send[q] = found.astype(BF)

                @pl.when(pos["z"] == q)
                def _(found=found):
                    z_own[...] = found

            for k in (1, 2, 3):
                along_z(k).start()

        def fifth():
            for k in (1, 2, 3):
                along_z(k).wait_recv()
            out_ref[...] = (z_own[...] + wide(z_recv.at[1]) + (wide(z_recv.at[2]) + wide(z_recv.at[3]))).astype(BF)
            for k in (1, 2, 3):
                along_z(k).wait_send()
            for p in range(4):
                for k in range(6):
                    copy(p, k).wait_send()

        return [zero, first, second, third, fourth, fifth]


class Fetch:
    def __init__(self, mine, at, done_z=False):
        r, cols = mine.shape
        self.at, self.pieces, self.done_z = at, pieces_of(cols), done_z
        self.args, self.specs = [mine], [pl.BlockSpec((r, cols), lambda *_: (0, 0))]
        r //= 4 if done_z else 1
        self.outs, self.out_specs = [jax.ShapeDtypeStruct((2, 4, 4, 4 * r, cols), BF)], [pl.BlockSpec(memory_space=pl.ANY)]
        self.scratch = [] if done_z else [pltpu.VMEM((4, r, cols), BF), pltpu.VMEM((4 * r, cols), F32), pltpu.VMEM((4 * r, cols), BF)]
        self.scratch += [pltpu.SemaphoreType.DMA((43,)), pltpu.SemaphoreType.DMA((43,)), pltpu.SemaphoreType.DMA((1,))]

    def events(self, ins, outs, scratch):
        (mine,), (w,) = ins, outs
        send, recv, local = scratch[-3:]
        four, wide, block = (None, None, mine) if self.done_z else scratch[:3]
        sems, pos, r = (send, recv), place(), mine.shape[0]
        which = lax.axis_index("rep")

        def one(p, t):
            a, _, _, c0, c = self.pieces[p]
            return w.at[which, t, pos["y"], :, pl.ds(c0, c)] if a == "x" else w.at[which, pos["x"], t, :, pl.ds(c0, c)]

        def row(p, t):
            a, _, _, c0, c = self.pieces[p]
            return w.at[which, :, t, :, pl.ds(c0, c)] if a == "x" else w.at[which, t, :, :, pl.ds(c0, c)]

        def copy(p, k):
            a, b, s, _, _ = self.pieces[p]
            if k < 3:
                ref, where = one(p, mod(pos[a] + (0, 0, -s)[k])), near(a, (1, -1, s)[k])
            elif k < 6:
                ref, where = row(p, mod(pos[b] + (0, 0, -s)[k - 3])), near(b, (1, -1, s)[k - 3])
            else:
                ref, where = row(p, mod(pos[b] + (0, 1, -1, 2)[k - 6])), peer()
            return remote(sems, 10 * p + k, ref, ref, where)

        def along_z(k):
            return remote(sems, 39 + k, mine, four.at[pos["z"]], near("z", k))

        def zero():
            if self.done_z:
                return
            for k in (1, 2, 3):
                along_z(k).start()
            four[pos["z"]] = mine[...]

        def first():
            if not self.done_z:
                for k in (1, 2, 3):
                    along_z(k).wait_recv()
                for q in range(4):
                    wide[pl.ds(r * q, r), :] = four[q].astype(F32)
                block[...] = wide[...].astype(BF)
            own = pltpu.make_async_copy(block, w.at[which, pos["x"], pos["y"]], local.at[0])
            own.start()
            own.wait()
            for p in range(4):
                copy(p, 0).start()
                copy(p, 1).start()

        def second():
            for p in range(4):
                copy(p, 0 if self.pieces[p][2] > 0 else 1).wait_recv()
                copy(p, 2).start()

        def third():
            for p in range(4):
                copy(p, 1 if self.pieces[p][2] > 0 else 0).wait_recv()
                copy(p, 2).wait_recv()
                for k in (3, 4, 6):
                    copy(p, k).start()

        def fourth():
            for p in range(4):
                up = self.pieces[p][2] > 0
                copy(p, 3 if up else 4).wait_recv()
                copy(p, 5).start()
                copy(p, 8 if up else 7).start()

        def fifth():
            for p in range(4):
                up = self.pieces[p][2] > 0
                copy(p, 4 if up else 3).wait_recv()
                copy(p, 7 if up else 8).start()
            for p in range(4):
                copy(p, 5).wait_recv()
                copy(p, 9).start()

        def sixth():
            for k in () if self.done_z else (1, 2, 3):
                along_z(k).wait_send()
            for p in range(4):
                for k in range(6, 10):
                    copy(p, k).wait_recv()
                for k in range(10):
                    copy(p, k).wait_send()

        return [zero, first, second, third, fourth, fifth, sixth]


class Along:
    def __init__(self, mine, at):
        r, cols = mine.shape
        self.at = at
        self.args, self.specs = [mine], [pl.BlockSpec((r, cols), lambda *_: (0, 0))]
        self.outs, self.out_specs = [jax.ShapeDtypeStruct((4 * r, cols), BF)], [pl.BlockSpec((4 * r, cols), lambda *_: (0, 0))]
        self.scratch = [pltpu.VMEM((4, r, cols), BF), pltpu.VMEM((4 * r, cols), F32)]
        self.scratch += [pltpu.SemaphoreType.DMA((3,)), pltpu.SemaphoreType.DMA((3,))]

    def events(self, ins, outs, scratch):
        (mine,), (block,) = ins, outs
        four, wide, *sems = scratch
        z, r = place()["z"], mine.shape[0]

        def along_z(k):
            return remote(sems, k - 1, mine, four.at[z], near("z", k))

        def zero():
            for k in (1, 2, 3):
                along_z(k).start()
            four[z] = mine[...]

        def first():
            for k in (1, 2, 3):
                along_z(k).wait_recv()
            for q in range(4):
                wide[pl.ds(r * q, r), :] = four[q].astype(F32)
            block[...] = wide[...].astype(BF)
            for k in (1, 2, 3):
                along_z(k).wait_send()

        return [zero, first]


def run(body, grid, args, in_specs, outs, out_specs, scratch=(), comms=(), cid=None, flops=0, name=None):
    ni, no, ns = len(args), len(outs), len(scratch)
    args, in_specs, outs, out_specs, scratch = list(args), list(in_specs), list(outs), list(out_specs), list(scratch)
    spans = []
    for one in comms:
        lengths = [len(v) for v in (args, outs, scratch)]
        args += one.args
        in_specs += one.specs
        outs += one.outs
        out_specs += one.out_specs
        scratch += one.scratch
        spans.append([slice(lo, len(v)) for lo, v in zip(lengths, (args, outs, scratch))])

    def kernel(*refs):
        ins, os, sc = refs[: len(args)], refs[len(args) : len(args) + len(outs)], refs[len(args) + len(outs) :]
        step = 0
        for d, n in enumerate(grid):
            step = step * n + pl.program_id(d)
        todo = []
        for one, (i, o, c) in zip(comms, spans):
            todo.append(list(zip(one.at, one.events(ins[i], os[o], sc[c]), strict=True)))
        if comms:
            pl.when(step == 0)(greet)
        for n in range(max([len(t) for t in todo], default=0)):
            for t in todo:
                if n < len(t):
                    pl.when(step == t[n][0])(t[n][1])
        if body is not None:
            body(*ins[:ni], *os[:no], *sc[:ns])

    params = dict(dimension_semantics=("arbitrary",) * len(grid), vmem_limit_bytes=LIMIT)
    if comms:
        params.update(collective_id=cid, has_side_effects=True)
    return pl.pallas_call(
        kernel,
        grid=grid,
        in_specs=in_specs,
        out_shape=outs,
        out_specs=out_specs,
        scratch_shapes=scratch,
        compiler_params=pltpu.CompilerParams(**params),
        cost_estimate=pl.CostEstimate(flops=flops, bytes_accessed=flops // 500, transcendentals=0),
        name=name,
    )(*args)


def S(shape, dtype=BF):
    return jax.ShapeDtypeStruct(shape, dtype)


def valid(shape, axis, tile, size):
    return lax.broadcasted_iota(jnp.int32, shape, axis) < size - tile * TF


def gate_up_specs(d):
    return [pl.BlockSpec((None, d, TF), lambda j, i, k=k: (k, 0, j)) for k in range(2)]


def prepared(h, **comm):
    t, d = h.shape

    def body(h_ref, a_ref, at_ref):
        wide = h_ref[...].astype(F32)
        scale = lax.rsqrt(jnp.mean(wide * wide, -1, keepdims=True) + 1e-6)
        a = (wide * scale).astype(BF)
        a_ref[...] = a
        at_ref[...] = a.T

    rows = pl.BlockSpec((TT, d), lambda i: (i, 0))
    return run(body, (t // TT,), (h,), [rows], [S((t, d)), S((d, t))], [rows, pl.BlockSpec((d, TT), lambda i: (0, i))], flops=4000 * t, name="prepared", **comm)


def act_of(a, wgu, **comm):
    (t, d), f = a.shape, wgu.shape[2]
    nf, tile = -(-f // TF), 2 * TT

    def body(a_ref, g_ref, u_ref, o_ref):
        j = pl.program_id(0)
        for k in range(2):
            rows = pl.ds(k * TT, TT)
            gate, up = dot(a_ref[rows, :], g_ref[...]), dot(a_ref[rows, :], u_ref[...])
            act = jax.nn.silu(gate) * up
            o_ref[rows, :] = jnp.where(valid(act.shape, 1, j, f), act, 0.0).astype(BF)

    return run(body, (nf, t // tile), (a, wgu, wgu), [pl.BlockSpec((tile, d), lambda j, i: (i, 0)), *gate_up_specs(d)], [S((t, nf * TF))], [pl.BlockSpec((tile, TF), lambda j, i: (i, j))], flops=4 * t * d * f, name="act", **comm)


def down_of(act, wd, number, h, **comm):
    t, d, f = act.shape[0], h.shape[1], wd.shape[1]
    nf, nt = act.shape[1] // TF, t // TT

    def body(a_ref, w_ref, h_ref, o_ref, acc):
        j, i = pl.program_id(0), pl.program_id(1)
        rows = pl.ds(i * TT, TT)

        def add(w):
            got = dot(a_ref[...], w)
            acc[rows, :] = jnp.where(j == 0, got, acc[rows, :] + got)

        @pl.when(j < nf - 1)
        def _():
            add(w_ref[...])

        @pl.when(j == nf - 1)
        def _():
            add(jnp.where(valid((TF, d), 0, j, f), w_ref[...], jnp.zeros((), BF)))
            o_ref[...] = (h_ref[...].astype(F32) + acc[rows, :].astype(BF).astype(F32)).astype(BF)

    last = lambda j, i: (jnp.where(j == nf - 1, i, 0), 0)
    return run(
        body, (nf, nt), (act, wd, h),
        [pl.BlockSpec((TT, TF), lambda j, i: (i, j)), pl.BlockSpec((None, TF, d), lambda j, i: (number, j, 0)), pl.BlockSpec((TT, d), last)],
        [S((t, d))], [pl.BlockSpec((TT, d), last)], [pltpu.VMEM((t, d), F32)], flops=2 * t * d * f, name="down", **comm,
    )


def back_act(a, wgu, dh, wd, number, tile=TT, **comm):
    (t, d), f = a.shape, wgu.shape[2]
    nf = -(-f // TF)

    def body(a_ref, g_ref, u_ref, dh_ref, w_ref, at_ref, dg_ref, du_ref):
        j = pl.program_id(0)
        for k in range(tile // TT):
            rows = pl.ds(k * TT, TT)
            gate, up = dot(a_ref[rows, :], g_ref[...]), dot(a_ref[rows, :], u_ref[...])
            by = dot(dh_ref[rows, :], w_ref[...], NT).astype(BF).astype(F32)
            s = jax.nn.sigmoid(gate)
            silu = gate * s
            at_ref[:, rows] = (silu * up).astype(BF).T
            ok = valid(by.shape, 1, j, f)
            dg_ref[rows, :] = jnp.where(ok, by * up * (s * (1 + gate * (1 - s))), 0.0).astype(BF)
            du_ref[rows, :] = jnp.where(ok, by * silu, 0.0).astype(BF)

    rows = pl.BlockSpec((tile, d), lambda j, i: (i, 0))
    out = pl.BlockSpec((tile, TF), lambda j, i: (i, j))
    return run(
        body, (nf, t // tile), (a, wgu, wgu, dh, wd), [rows, *gate_up_specs(d), rows, pl.BlockSpec((None, TF, d), lambda j, i: (number, j, 0))],
        [S((f, t)), S((t, nf * TF)), S((t, nf * TF))], [pl.BlockSpec((TF, tile), lambda j, i: (j, i)), out, out],
        flops=6 * t * d * f, name="back_act", **comm,
    )


def back_in(dg, du, wgu, h, dh, **comm):
    t, (_, d, f) = dg.shape[0], wgu.shape
    nf, nt = dg.shape[1] // TF, t // TT

    def body(dg_ref, du_ref, g_ref, u_ref, h_ref, dh_ref, o_ref, acc):
        j, i = pl.program_id(0), pl.program_id(1)
        rows = pl.ds(i * TT, TT)

        def add(g, u):
            got = dot(dg_ref[...], g, NT) + dot(du_ref[...], u, NT)
            acc[rows, :] = jnp.where(j == 0, got, acc[rows, :] + got)

        @pl.when(j < nf - 1)
        def _():
            add(g_ref[...], u_ref[...])

        @pl.when(j == nf - 1)
        def _():
            ok, zero = valid((d, TF), 1, j, f), jnp.zeros((), BF)
            add(jnp.where(ok, g_ref[...], zero), jnp.where(ok, u_ref[...], zero))
            by = acc[rows, :].astype(BF).astype(F32)
            wide = h_ref[...].astype(F32)
            scale = lax.rsqrt(jnp.mean(wide * wide, -1, keepdims=True) + 1e-6)
            along = jnp.sum(by * wide, -1, keepdims=True)
            own = by * scale - wide * (along * (scale * scale * scale) * (1.0 / d))
            o_ref[...] = (dh_ref[...].astype(F32) + own.astype(BF).astype(F32)).astype(BF)

    last = lambda j, i: (jnp.where(j == nf - 1, i, 0), 0)
    tile, out = pl.BlockSpec((TT, TF), lambda j, i: (i, j)), pl.BlockSpec((TT, d), last)
    return run(body, (nf, nt), (dg, du, wgu, wgu, h, dh), [tile, tile, *gate_up_specs(d), out, out], [S((t, d))], [out], [pltpu.VMEM((t, d), F32)], flops=4 * t * d * f, name="back_in", **comm)


def weights_in(a_t, dg, du, f, **comm):
    d, t = a_t.shape
    nf, half = dg.shape[1] // TF, d // 2

    def body(a_ref, g_ref, u_ref, og_ref, ou_ref):
        @pl.when(pl.program_id(0) < nf)
        def _():
            og_ref[...] = dot(a_ref[...], g_ref[...]).astype(BF)

        @pl.when(pl.program_id(0) >= nf)
        def _():
            ou_ref[...] = dot(a_ref[...], u_ref[...]).astype(BF)

    gate = lambda j: jnp.minimum(j, nf - 1)
    up = lambda j: jnp.maximum(j - nf, 0)
    return run(
        body, (2 * nf, 2), (a_t, dg, du),
        [pl.BlockSpec((half, t), lambda j, i: (i, 0)), pl.BlockSpec((t, TF), lambda j, i: (0, gate(j))), pl.BlockSpec((t, TF), lambda j, i: (0, up(j)))],
        [S((d, f)), S((d, f))],
        [pl.BlockSpec((half, TF), lambda j, i: (jnp.where(j < nf, i, 1), gate(j))), pl.BlockSpec((half, TF), lambda j, i: (jnp.where(j < nf, 0, i), up(j)))],
        flops=4 * t * d * f, name="weights_in", **comm,
    )


def weights_out(act_t, dh, **comm):
    f, t = act_t.shape
    d, tile = dh.shape[1], 320

    def body(a_ref, b_ref, o_ref):
        o_ref[...] = dot(a_ref[...], b_ref[...]).astype(BF)

    return run(body, (f // tile,), (act_t, dh), [pl.BlockSpec((tile, t), lambda j: (j, 0)), pl.BlockSpec((t, d), lambda j: (0, 0))], [S((f, d))], [pl.BlockSpec((tile, d), lambda j: (j, 0))], flops=2 * t * d * f, name="weights_out", **comm)


NAMES = ("w_gate", "w_up", "w_down")


def normed(h):
    wide = h.astype(F32)
    scale = lax.rsqrt(jnp.mean(wide**2, -1, keepdims=True) + 1e-6)
    return (wide * scale).astype(BF)


def adamw(w, m, v, g):
    m = 0.9 * m + 0.1 * g
    v = 0.95 * v + 0.05 * g * g
    step = m * lax.rsqrt(v + 1e-8) + 0.1 * w
    return (w - 0.02 * step).astype(BF), m, v


def solution(mesh):
    def step(x, dy, *arrays):
        weights, m, v = (arrays[i : i + 3] for i in (0, 3, 6))
        first = lax.axis_index("rep") == 0
        f = weights[0].shape[2]

        def gate_up(number):
            return jnp.where(first, weights[0][number], weights[1][number])

        def whole(w):
            return w.reshape(2, -1, w.shape[-1])

        downs = jnp.where(first, weights[2][0], weights[2][1])
        h0, dh2 = x[0], dy[0]
        now = [Fetch(gate_up(0), (0, 3, 3, 3, 3, 3, 3)), Along(downs, (0, 3)), Along(gate_up(1), (0, 3))]
        a0, a0_t, wgu0, downs, later = prepared(h0, comms=now, cid=1)
        wgu0 = whole(wgu0)
        act0, wd = act_of(a0, wgu0, comms=[Fetch(downs, (0, 0, 2, 4, 10, 11, 11), True)], cid=2)
        wd = whole(wd)
        h1, wgu1 = down_of(act0, wd, 0, h0, comms=[Fetch(later, (0, 0, 7, 11, 23, 23, 23), True)], cid=3)
        wgu1 = whole(wgu1)
        a1, a1_t = prepared(h1)
        at1, dg1, du1 = back_act(a1, wgu1, dh2, wd, 1, 2 * TT)
        down1 = weights_out(at1, dh2)[0]
        gate1, up1, g_down1 = weights_in(a1_t, dg1, du1, f, comms=[Scatter(down1, (0, 5, 15, 17, 20, 23))], cid=4)
        dh1, g_gate1 = back_in(dg1, du1, wgu1, h1, dh2, comms=[Scatter(gate1, (0, 5, 15, 17, 20, 23))], cid=5)
        at0, dg0, du0, g_up1 = back_act(a0, wgu0, dh1, wd, 0, comms=[Scatter(up1, (0, 5, 14, 18, 20, 22))], cid=6)
        down0 = weights_out(at0, dh1)[0]
        gate0, up0, g_down0 = weights_in(a0_t, dg0, du0, f, comms=[Scatter(down0, (0, 5, 15, 17, 20, 23))], cid=7)
        g_gate0, g_up0 = run(None, (1,), (), [], [], [], comms=[Scatter(gate0, (0,) * 6), Scatter(up0, (0,) * 6)], cid=8, name="scatter")
        gradients = [jnp.stack(pair).astype(F32) for pair in ((g_gate0, g_gate1), (g_up0, g_up1), (g_down0, g_down1))]
        new = [adamw(w.astype(F32), m, v, g) for w, m, v, g in zip(weights, m, v, gradients, strict=True)]
        return tuple(one[which] for which in range(3) for one in new)

    states, cut = P(("rep", "dp"), None, None), P(None, "dp", None)
    return jax.shard_map(
        step,
        mesh=mesh,
        in_specs=(states, states) + (cut,) * 9,
        out_specs=(P("rep", "dp", None),) * 9,
        check_vma=False,
    )
```
